768 devices in a mesh: enc: 8 (over x, core), row: 24 (over z, y_hi), col: 4 (over y_lo).
Axes of the slice: x: 4, y: 8 (y_hi: 2, y_lo: 4; y = y_hi * 4 + y_lo), z: 12, core: 2. Of those that a mesh axis runs over, the one named last changes fastest.
Arguments:
- out_grad: bfloat16 [288, 8192], P(None, ('enc', 'col')), may hold values from -6 to 6
- gate_pre: bfloat16 [288, 29568], P('enc', 'row'), may hold values from -6 to 6
- up_pre: bfloat16 [288, 29568], P('enc', 'row'), may hold values from -6 to 6
- w_gate: bfloat16 [8192, 29568], P(('enc', 'col'), 'row'), may hold values from -0.0625 to 0.0625
- w_up: bfloat16 [8192, 29568], P(('enc', 'col'), 'row'), may hold values from -0.0625 to 0.0625
- w_down: bfloat16 [29568, 8192], P('row', ('enc', 'col')), may hold values from -0.03125 to 0.03125
- w_proj: bfloat16 [12800, 8192], P(None, ('enc', 'col')), may hold values from -0.0546875 to 0.0546875
- enc_hidden: bfloat16 [1152, 6400], P('row', ('enc', 'col')), may hold values from -6 to 6
- route: int32 [288], replicated, may hold values from 0 to 287, each once
- img_count: int32 [24], replicated, may hold values from 1 to 12
Outputs:
- enc_grad: bfloat16 [3200, 6400], P(None, ('enc', 'col'))
The draws below stay inside these ranges and needn't reach their ends.
Inputs may be any that keep to these rules, and one draw needn't show every extreme that they name: route[12 * r + k] is the language row that holds slot k of row group r; every language row appears once. Slots k of row group r with k >= img_count[r] are empty.
All inputs are finite; a program needn't handle non-finite values.
Results may differ from the reference program's by a relative error of at most 0.02.
Values may be sent and summed in bfloat16 or wider, within the bound.
A program may use at most 64 MiB of HBM per device.

```python
import math
import jax
import jax.numpy as jnp
from jax import lax

D = 8192
FF = 29568
VD = 3200
VF = 6400
SHUF = 4
IMG = 12
NI = 288
PATCH = 1152
PD = 12800
N_ROW = 24


def plant(values, rng, low, top_value):
    dims = values.shape
    index_at = [jax.random.randint(jax.random.fold_in(rng, axis), (), 0, dims[axis]) for axis in range(len(dims))]
    values = values.at[tuple(index_at)].set(low)
    longest = dims.index(max(dims))
    index_at[longest] = (index_at[longest] + 1) % dims[longest]
    return values.at[tuple(index_at)].set(top_value)


def block_scale(own_key, extent, cuts, low, largest):
    def one(dim, blocks):
        draws = jax.random.uniform(jax.random.fold_in(jax.random.fold_in(own_key, 6), dim), (blocks,), jnp.float32, low / len(cuts), largest / len(cuts))
        return jnp.repeat(jnp.exp(draws), extent[dim] // blocks).reshape((-1,) + (1,) * (len(extent) - dim - 1))

    level = one(*cuts[0])
    for cut in cuts[1:]:
        level = level * one(*cut)
    return level


def bell_draw(rng, extent, spread, limit, pieces=(), kind=jnp.bfloat16):
    level = block_scale(rng, extent, pieces, -0.22, 0.18) if pieces else 1.0
    result = jax.random.normal(rng, extent, jnp.float32) * spread * level
    return jnp.minimum(jnp.maximum(result, -limit), limit).astype(kind)


def setup_inputs(seed: int = 0) -> dict:
    splits = jax.random.split(jax.random.key(seed), 11)
    out_grad = bell_draw(splits[0], (NI, D), 1.0, 6.0, ((1, 32),))
    gate_pre = bell_draw(splits[1], (NI, FF), 1.0, 6.0, ((0, 8), (1, 24)))
    up_pre = bell_draw(splits[2], (NI, FF), 1.0, 6.0, ((0, 8), (1, 24)))
    w_gate = bell_draw(splits[3], (D, FF), D ** -0.5, 0.0625, ((0, 32), (1, 24)))
    w_up = bell_draw(splits[4], (D, FF), D ** -0.5, 0.0625, ((0, 32), (1, 24)))
    w_down = bell_draw(splits[5], (FF, D), FF ** -0.5, 0.03125, ((0, 24), (1, 32)))
    w_proj = bell_draw(splits[6], (PD, D), PD ** -0.5, 0.0546875, ((1, 32),))
    enc_hidden = bell_draw(splits[7], (PATCH, VF), 1.0, 6.0, ((0, 24), (1, 32)))
    route = jax.random.permutation(splits[8], NI).astype(jnp.int32)
    img_count = plant(jax.random.randint(splits[9], (N_ROW,), 1, IMG + 1), jax.random.fold_in(splits[9], 1), 1, IMG).astype(jnp.int32)
    return {"out_grad": out_grad, "gate_pre": gate_pre, "up_pre": up_pre, "w_gate": w_gate, "w_up": w_up, "w_down": w_down, "w_proj": w_proj, "enc_hidden": enc_hidden, "route": route, "img_count": img_count}


def reference(out_grad, gate_pre, up_pre, w_gate, w_up, w_down, w_proj, enc_hidden, route, img_count):
    hidden_grad = jnp.dot(out_grad, w_down.T, preferred_element_type=jnp.float32)
    gate_vals = gate_pre.astype(jnp.float32)
    up_vals = up_pre.astype(jnp.float32)
    squash = jax.nn.sigmoid(gate_vals)
    grad_gate = (hidden_grad * up_vals * squash * (1.0 + gate_vals * (1.0 - squash))).astype(jnp.bfloat16)
    grad_up = (hidden_grad * gate_vals * squash).astype(jnp.bfloat16)
    routed_gate = jnp.take(grad_gate, route, axis=0)
    routed_up = jnp.take(grad_up, route, axis=0)
    input_grad = jnp.dot(routed_gate, w_gate.T, preferred_element_type=jnp.float32) + jnp.dot(routed_up, w_up.T, preferred_element_type=jnp.float32)
    positions = jnp.arange(NI, dtype=jnp.int32)
    alive_mask = positions % IMG < jnp.repeat(img_count, IMG)
    image_grad = jnp.where(alive_mask[:, None], input_grad, jnp.zeros_like(input_grad)).astype(jnp.bfloat16)
    shuffled_grad = jnp.dot(image_grad, w_proj.T, preferred_element_type=jnp.float32)
    patch_grad = shuffled_grad.reshape(NI, VD, SHUF).transpose(0, 2, 1).reshape(PATCH, VD).astype(jnp.bfloat16)
    hidden_groups = enc_hidden.reshape(N_ROW, SHUF * IMG, VF)
    grad_groups = patch_grad.reshape(N_ROW, SHUF * IMG, VD)
    scale = 1.0 / math.sqrt(PATCH)

    def add_group(total, pair):
        term = lax.dot_general(pair[1], pair[0], (((0,), (0,)), ((), ())), preferred_element_type=jnp.float32) * scale
        rounded = lax.optimization_barrier(term.astype(jnp.bfloat16))
        return (total + rounded.astype(jnp.float32), None)
    total, unused = lax.scan(add_group, jnp.zeros((VD, VF), jnp.float32), (hidden_groups, grad_groups))
    return total.astype(jnp.bfloat16)
```

```python
import functools
import math

import jax
import jax.numpy as jnp
from jax import lax
from jax.experimental import pallas as pl
from jax.experimental.pallas import tpu as pltpu
from jax.sharding import PartitionSpec as P

F32 = jnp.float32
BF16 = jnp.bfloat16
MESH = pl.DeviceIdType.MESH

NI = 288
ROWT = NI // 16
KD = 256
HID = 1232
HIDP = 1280
LT = HIDP // 128
GR = 36
GRP = 80
EC = 200
HT = 192
YT = 96
IMG = 12
PATCH = 1152
FT = 128
PIECE = 224
LAG = 2


def dot_nt(a, b):
    return lax.dot_general(a, b, (((1,), (1,)), ((), ())), preferred_element_type=F32)


def dot_nn(a, b):
    return lax.dot_general(a, b, (((1,), (0,)), ((), ())), preferred_element_type=F32)


def iota(shape, dim):
    return lax.broadcasted_iota(jnp.int32, shape, dim)


def onehot(pred):
    return jnp.where(pred, jnp.float32(1), jnp.float32(0)).astype(BF16)


def await_bytes(ref, sem):
    pltpu.make_async_copy(ref, ref, sem).wait()


def kernel(
    og_h, g_h, u_h, wg_h, wu_h, wd_h, wp_h, eh_h, rt, cnt, out,
    og, wd, wg, wu, wpm, wpp, graw, uraw, eraw, gpad, upad,
    gu, ebuf, hbuf, ra1, s1, ra2, s2, ra3, hfull, fa, fb,
    xb, rb1, sb, rb2, xfull, ept,
    yb, rc1, c1, rc2, c2, yfull, fin,
    lsem, ssem, rsem,
):
    e, r, c = lax.axis_index("enc"), lax.axis_index("row"), lax.axis_index("col")
    x, core = e // 2, e % 2
    z, yh = r // 2, r % 2

    sib = (x * 2 + (1 - core), r, c)
    other_y = (e, z * 2 + (1 - yh), c)

    def at_x(k):
        return lax.rem(x + k, 4)

    def at_c(k):
        return lax.rem(c + k, 4)

    def at_z(k):
        return lax.rem(z + k, 12)

    def dev_x(k):
        return (at_x(k) * 2 + core, r, c)

    def dev_c(k):
        return (e, r, at_c(k))

    def dev_z(k):
        return (e, at_z(k) * 2 + yh, c)

    def send(src, dst, n, to):
        pltpu.make_async_remote_copy(
            src_ref=src, dst_ref=dst, send_sem=ssem.at[n], recv_sem=rsem.at[n],
            device_id=to, device_id_type=MESH,
        ).start()

    def local(src, dst, n):
        copy = pltpu.make_async_copy(src, dst, lsem.at[n])
        copy.start()
        return copy

    wp_main = wp_h.at[pl.ds(pl.multiple_of(r * 512, 512), 512)]
    wp_tail = wp_h.at[pl.ds(pl.multiple_of(12288 + 32 * jnp.minimum(r, 15), 32), 32)]
    load_og = local(og_h, og, 0)
    load_wd = local(wd_h, wd.at[pl.ds(0, HID)], 1)
    load_g = local(g_h, graw, 2)
    load_u = local(u_h, uraw, 3)
    load_e = local(eh_h, eraw, 4)
    load_wg = local(wg_h, wg.at[pl.ds(0, HID)], 5)
    load_wu = local(wu_h, wu.at[pl.ds(0, HID)], 6)
    load_wm = local(wp_main, wpm.at[pl.ds(0, 512)], 7)
    load_wt = local(wp_tail, wpm.at[pl.ds(512, 32)], 8)

    barrier = pltpu.get_barrier_semaphore()
    pl.semaphore_signal(barrier, inc=1, device_id=sib, device_id_type=MESH)
    pl.semaphore_signal(barrier, inc=1, device_id=other_y, device_id_type=MESH)
    for k in range(1, 4):
        pl.semaphore_signal(barrier, inc=1, device_id=dev_x(k), device_id_type=MESH)
        pl.semaphore_signal(barrier, inc=1, device_id=dev_c(k), device_id_type=MESH)
    for k in range(1, 12):
        pl.semaphore_signal(barrier, inc=1, device_id=dev_z(k), device_id_type=MESH)

    tail = jnp.zeros((HIDP - HID, KD), BF16)
    wd[HID:, :] = tail
    wg[HID:, :] = tail
    wu[HID:, :] = tail
    gpad[...] = jnp.zeros_like(gpad)
    upad[...] = jnp.zeros_like(upad)
    hbuf[ROWT * LT :] = jnp.zeros((HT - ROWT * LT, 16, 128), BF16)
    yb[ROWT * 5 :] = jnp.zeros((YT - ROWT * 5, 16, 128), BF16)
    ebuf[r] = jnp.zeros((48, 256), BF16)

    load_g.wait()
    load_u.wait()
    gpad[0:GR, 0:HID] = graw[...]
    upad[0:GR, 0:HID] = uraw[...]
    row, lane = iota((GRP, 48), 0), iota((GRP, 48), 1)
    pick_g = onehot((row == lane) & (lane < GR))
    pick_u = onehot((row == lane + GR) & (lane < GR))
    stacked = dot_nn(pick_g, gpad[...]) + dot_nn(pick_u, upad[...])
    stacked = stacked.astype(BF16)
    gu[0, x, core] = stacked[:, 0:640]
    gu[1, x, core] = stacked[:, 640:1280]
    load_e.wait()
    ebuf[r, :, 0:EC] = eraw[...]

    load_og.wait()
    load_wd.wait()

    def hidden(j, carry):
        w = wd[pl.ds(pl.multiple_of(j * 128, 128), 128), :]
        part = dot_nt(og[...], w)
        hbuf[pl.ds(j * ROWT, ROWT)] = part.reshape(ROWT, 16, 128).astype(BF16)
        return carry

    lax.fori_loop(0, LT, hidden, 0)

    pl.semaphore_wait(barrier, 19)

    half = HT // 2
    send(hbuf.at[pl.ds((1 - core) * half, half)], ra1, 0, sib)
    for k in range(1, 4):
        send(gu.at[0, x, core], gu.at[0, x, core], 10, dev_x(k))
    send(ebuf.at[r], ebuf.at[r], 12, other_y)
    await_bytes(ra1, rsem.at[0])
    mine = hbuf[pl.ds(core * half, half)].astype(F32) + ra1[...].astype(F32)
    s1[...] = mine.astype(BF16).reshape(4, 24, 16, 128)

    for k in range(1, 4):
        send(s1.at[at_x(k)], ra2.at[k - 1], 1, dev_x(k))
    for k in range(1, 4):
        send(gu.at[1, x, core], gu.at[1, x, core], 11, dev_x(k))
    await_bytes(ebuf.at[0], rsem.at[12])
    await_bytes(ebuf.at[0], ssem.at[12])
    pair = ebuf.at[pl.ds(2 * z, 2)]
    for k in range(1, 12):
        send(pair, pair, 13, dev_z(k))
    await_bytes(ra2, rsem.at[1])
    got = s1[x].astype(F32)
    for k in range(3):
        got = got + ra2[k].astype(F32)
    s2[...] = got.astype(BF16).reshape(4, 6, 16, 128)

    for k in range(1, 4):
        send(s2.at[at_c(k)], ra3.at[k - 1], 2, dev_c(k))

    load_wm.wait()
    load_wt.wait()
    for q in range(4):
        move = onehot(iota((128, 512), 1) == 4 * iota((128, 512), 0) + q)
        wpp[q * 128 : (q + 1) * 128, :] = dot_nn(move, wpm[0:512, :]).astype(BF16)
    row, lane = iota((128, 32), 0), iota((128, 32), 1)
    move = onehot((lane == 4 * (row & 7) + (row >> 3)) & (row < 32))
    wpp[512:640, :] = dot_nn(move, wpm[512:544, :]).astype(BF16)

    await_bytes(ra3, rsem.at[2])
    got = s2[c].astype(F32)
    for k in range(3):
        got = got + ra3[k].astype(F32)
    base = core * half + x * 24
    hfull[pl.ds(base + c * 6, 6)] = got.astype(BF16)

    own = hfull.at[pl.ds(base + c * 6, 6)]
    for k in range(1, 4):
        send(own, own, 3, dev_c(k))
    await_bytes(gu.at[0, pl.ds(0, 3), 0], rsem.at[10])
    await_bytes(gu.at[0, pl.ds(0, 3), 0], rsem.at[11])
    await_bytes(gu.at[0, pl.ds(0, 3), 0], ssem.at[10])
    await_bytes(gu.at[0, pl.ds(0, 3), 0], ssem.at[11])
    send(gu.at[:, :, core], gu.at[:, :, core], 14, sib)
    await_bytes(hfull.at[pl.ds(0, 18)], rsem.at[3])
    await_bytes(hfull.at[pl.ds(0, 18)], ssem.at[3])
    own = hfull.at[pl.ds(base, 24)]
    for k in range(1, 4):
        send(own, own, 4, dev_x(k))

    await_bytes(gu.at[:, :, 0], rsem.at[14])
    await_bytes(gu.at[:, :, 0], ssem.at[14])
    col = iota((NI, 8 * GRP), 1)
    target = col
    for s in range(1, 8):
        target = target - jnp.where(col >= GRP * s, GRP - GR, 0)
    start_of = jnp.zeros_like(col)
    for s in range(1, 8):
        start_of = start_of + jnp.where(col >= GRP * s, GRP, 0)
    within = col - start_of
    row = iota((NI, 8 * GRP), 0)
    place_g = onehot((row == target) & (within < GR))
    place_u = onehot((row == target - GR) & (within >= GR) & (within < 2 * GR))

    for h in range(2):
        def factors(j, carry):
            rows = gu[h, :, :, :, pl.ds(pl.multiple_of(j * 128, 128), 128)]
            rows = rows.reshape(8 * GRP, 128)
            gate = dot_nn(place_g, rows)
            up = dot_nn(place_u, rows)
            squash = 1.0 / (1.0 + jnp.exp(-gate))
            fa[h * 5 + j] = up * squash * (1.0 + gate * (1.0 - squash))
            fb[h * 5 + j] = gate * squash
            return carry

        lax.fori_loop(0, 5, factors, 0)

    await_bytes(hfull.at[pl.ds(0, 72)], rsem.at[4])
    await_bytes(hfull.at[pl.ds(0, 72)], ssem.at[4])
    own = hfull.at[pl.ds(core * half, half)]
    send(own, own, 5, sib)
    load_wg.wait()
    load_wu.wait()
    await_bytes(hfull.at[pl.ds(0, half)], rsem.at[5])
    await_bytes(hfull.at[pl.ds(0, half)], ssem.at[5])

    def inputs(j, total):
        h = hfull[pl.ds(j * ROWT, ROWT)].astype(F32).reshape(NI, 128)
        cut = pl.ds(pl.multiple_of(j * 128, 128), 128)
        total = total + dot_nn((h * fa[j]).astype(BF16), wg[cut, :])
        return total + dot_nn((h * fb[j]).astype(BF16), wu[cut, :])

    part = lax.fori_loop(0, LT, inputs, jnp.zeros((NI, KD), F32))
    for l in range(2):
        xb[l * 36 : (l + 1) * 36] = part[:, l * 128 : (l + 1) * 128].reshape(36, 8, 128).astype(BF16)

    for k in range(1, 12):
        send(xb.at[pl.ds(at_z(k) * 6, 6)], rb1.at[k - 1], 6, dev_z(k))

    await_bytes(ebuf.at[pl.ds(0, 22)], rsem.at[13])
    await_bytes(ebuf.at[pl.ds(0, 22)], ssem.at[13])
    lane = iota((1, NI), 1)
    limit = jnp.zeros((1, NI), jnp.int32)
    for s in range(24):
        inside = (lane >= s * IMG) & (lane < (s + 1) * IMG)
        limit = jnp.where(inside, s * IMG + cnt[s], limit)
    slot_row = jnp.where(lane < limit, rt[...], -1)
    routed = onehot(iota((NI, NI), 0) == slot_row)
    et = ebuf[...].reshape(PATCH, 256).astype(F32).T.astype(BF16)
    for q in range(4):
        take = onehot(iota((PATCH, NI), 0) == 4 * iota((PATCH, NI), 1) + q)
        plane = dot_nn(et, take).astype(BF16)
        ept[q] = dot_nt(plane, routed).astype(BF16)

    await_bytes(rb1, rsem.at[6])
    got = xb[pl.ds(z * 6, 6)].astype(F32)
    for k in range(11):
        got = got + rb1[k].astype(F32)
    sb[...] = got.astype(BF16)
    send(sb, rb2, 7, other_y)
    await_bytes(rb2, rsem.at[7])
    xfull[pl.ds(z * 6, 6)] = (sb[...].astype(F32) + rb2[...].astype(F32)).astype(BF16)
    own = xfull.at[pl.ds(z * 6, 6)]
    for k in range(1, 12):
        send(own, own, 8, dev_z(k))
    await_bytes(xfull.at[pl.ds(0, 66)], rsem.at[8])
    await_bytes(xfull.at[pl.ds(0, 66)], ssem.at[8])

    both = xfull[...].astype(F32)
    left = both[0:36].reshape(NI, 128).astype(BF16)
    right = both[36:72].reshape(NI, 128).astype(BF16)
    for q in range(5):
        w = wpp[q * 128 : (q + 1) * 128, :]
        part = dot_nt(left, w[:, 0:128]) + dot_nt(right, w[:, 128:256])
        yb[q * ROWT : (q + 1) * ROWT] = part.reshape(ROWT, 16, 128).astype(BF16)

    half = YT // 2
    send(yb.at[pl.ds((1 - core) * half, half)], rc1, 9, sib)
    await_bytes(rc1, rsem.at[9])
    mine = yb[pl.ds(core * half, half)].astype(F32) + rc1[...].astype(F32)
    c1[...] = mine.astype(BF16).reshape(4, 12, 16, 128)
    for k in range(1, 4):
        send(c1.at[at_x(k)], rc2.at[k - 1], 15, dev_x(k))
    await_bytes(rc2, rsem.at[15])
    got = c1[x].astype(F32)
    for k in range(3):
        got = got + rc2[k].astype(F32)
    c2[c] = got.astype(BF16)
    for k in range(1, 4):
        send(c2.at[c], c2.at[c], 16, dev_c(k))
    await_bytes(c2.at[pl.ds(0, 3)], rsem.at[16])
    got = c2[0].astype(F32)
    for k in range(1, 4):
        got = got + c2[k].astype(F32)
    base = core * half + x * 12
    yfull[pl.ds(base, 12)] = got.astype(BF16)
    own = yfull.at[pl.ds(base, 12)]
    for k in range(1, 4):
        send(own, own, 17, dev_x(k))
    await_bytes(yfull.at[pl.ds(0, 36)], rsem.at[17])
    await_bytes(yfull.at[pl.ds(0, 36)], ssem.at[17])
    own = yfull.at[pl.ds(core * half, half)]
    send(own, own, 18, sib)
    await_bytes(yfull.at[pl.ds(0, half)], rsem.at[18])
    await_bytes(yfull.at[pl.ds(0, half)], ssem.at[18])

    scale = 1.0 / math.sqrt(PATCH)
    extra = yfull[4 * ROWT : 5 * ROWT].reshape(NI, 128)
    main = jnp.zeros((256, FT), F32)
    small = jnp.zeros((256, FT), F32)
    for q in range(4):
        main = main + dot_nn(ept[q], yfull[q * ROWT : (q + 1) * ROWT].reshape(NI, 128))
        tail = dot_nn(ept[q], extra)
        small = small + (tail if q == 0 else pltpu.roll(tail, 128 - 8 * q, 1))
    fin[r, 0:208] = (main[0:208] * scale).astype(BF16)
    turned = (small * scale).T
    fin[r, 208:224] = jnp.concatenate([turned[0:8, 0:128], turned[0:8, 128:256]], axis=0).astype(BF16)

    send(fin.at[r], fin.at[r], 19, other_y)

    def ring(n, flow, step, sign):
        piece = fin.at[lax.rem(z + 12 - sign * step, 12) * 2 + flow]
        send(piece, piece, n, dev_z(1 if sign > 0 else 11))

    flows = (yh, 1 - yh)
    first = 20

    def number(f, step, way):
        return first + (f * 6 + step) * 2 + way

    def begin(f):
        ring(number(f, 0, 0), flows[f], 0, 1)
        ring(number(f, 0, 1), flows[f], 0, -1)

    def forward(f, step):
        for way in range(2):
            if step >= 6 - way:
                continue
            n = number(f, step, way)
            await_bytes(fin.at[0], rsem.at[n])
            if step + 1 < 6 - way:
                ring(number(f, step + 1, way), flows[f], step + 1, 1 - 2 * way)

    begin(0)
    for step in range(6 + LAG):
        if step == LAG:
            await_bytes(fin.at[0], rsem.at[19])
            await_bytes(fin.at[0], ssem.at[19])
            begin(1)
        if step < 6:
            forward(0, step)
        if step >= LAG:
            forward(1, step - LAG)

    for s in range(24):
        out[:, s * 128 : (s + 1) * 128] = fin[s, 0:EC]
    ends = [jnp.concatenate([fin[s, 208:216], fin[s, 216:224]], axis=1).astype(F32) for s in range(16)]
    out[:, 3072:3200] = jnp.concatenate(ends, axis=0).T[0:EC].astype(BF16)

    await_bytes(ra1, ssem.at[0])
    await_bytes(ra2, ssem.at[1])
    await_bytes(ra3, ssem.at[2])
    await_bytes(rb1, ssem.at[6])
    await_bytes(rb2, ssem.at[7])
    await_bytes(rc1, ssem.at[9])
    await_bytes(rc2, ssem.at[15])
    await_bytes(c2.at[pl.ds(0, 3)], ssem.at[16])
    for f in range(2):
        for step in range(6):
            for way in range(2):
                if way == 1 and step == 5:
                    continue
                await_bytes(fin.at[0], ssem.at[number(f, step, way)])


def shards(out_grad, gate_pre, up_pre, w_gate, w_up, w_down, w_proj, enc_hidden, route, img_count):
    any_spec = pl.BlockSpec(memory_space=pl.ANY)
    vmem = pltpu.VMEM
    tile = (16, 128)
    n_sem = 20 + 24
    result = pl.pallas_call(
        kernel,
        out_shape=jax.ShapeDtypeStruct((EC, 3200), BF16),
        in_specs=[any_spec] * 8
        + [pl.BlockSpec(memory_space=pltpu.VMEM), pl.BlockSpec(memory_space=pltpu.SMEM)],
        out_specs=pl.BlockSpec(memory_space=pltpu.VMEM),
        scratch_shapes=[
            vmem((NI, KD), BF16),
            vmem((HIDP, KD), BF16),
            vmem((HIDP, KD), BF16),
            vmem((HIDP, KD), BF16),
            vmem((544, KD), BF16),
            vmem((640, KD), BF16),
            vmem((GR, HID), BF16),
            vmem((GR, HID), BF16),
            vmem((48, EC), BF16),
            vmem((48, HIDP), BF16),
            vmem((48, HIDP), BF16),
            vmem((2, 4, 2, GRP, 640), BF16),
            vmem((24, 48, 256), BF16),
            vmem((HT, *tile), BF16),
            vmem((HT // 2, *tile), BF16),
            vmem((4, 24, *tile), BF16),
            vmem((3, 24, *tile), BF16),
            vmem((4, 6, *tile), BF16),
            vmem((3, 6, *tile), BF16),
            vmem((HT, *tile), BF16),
            vmem((LT, NI, 128), F32),
            vmem((LT, NI, 128), F32),
            vmem((72, 8, 128), BF16),
            vmem((11, 6, 8, 128), BF16),
            vmem((6, 8, 128), BF16),
            vmem((6, 8, 128), BF16),
            vmem((72, 8, 128), BF16),
            vmem((4, 256, NI), BF16),
            vmem((YT, *tile), BF16),
            vmem((YT // 2, *tile), BF16),
            vmem((4, 12, *tile), BF16),
            vmem((3, 12, *tile), BF16),
            vmem((4, 12, *tile), BF16),
            vmem((YT, *tile), BF16),
            vmem((24, PIECE, 128), BF16),
            pltpu.SemaphoreType.DMA((9,)),
            pltpu.SemaphoreType.DMA((n_sem,)),
            pltpu.SemaphoreType.DMA((n_sem,)),
        ],
        compiler_params=pltpu.CompilerParams(
            collective_id=0, has_side_effects=True, vmem_limit_bytes=56 * 1024 * 1024
        ),
    )(
        out_grad, gate_pre, up_pre, w_gate.T, w_up.T, w_down, w_proj, enc_hidden,
        route.reshape(1, NI), img_count,
    )
    return result.T


def solution(mesh):
    placed = (
        P(None, ("enc", "col")),
        P("enc", "row"),
        P("enc", "row"),
        P(("enc", "col"), "row"),
        P(("enc", "col"), "row"),
        P("row", ("enc", "col")),
        P(None, ("enc", "col")),
        P("row", ("enc", "col")),
        P(),
        P(),
    )
    return jax.shard_map(
        shards, mesh=mesh, in_specs=placed, out_specs=P(None, ("enc", "col")), check_vma=False
    )
```

```python
import functools
import math

import jax
import jax.numpy as jnp
from jax import lax
from jax.experimental import pallas as pl
from jax.experimental.pallas import tpu as pltpu
from jax.sharding import PartitionSpec as P

F32 = jnp.float32
BF16 = jnp.bfloat16
MESH = pl.DeviceIdType.MESH

NI = 288
ROWT = NI // 16
KD = 256
HID = 1232
HIDP = 1280
LT = HIDP // 128
GR = 36
GRP = 80
EC = 200
HT = 192
YT = 96
IMG = 12
PATCH = 1152
FT = 128
PIECE = 224
CUT = PIECE // 2
LAG = 2


def dot_nt(a, b):
    return lax.dot_general(a, b, (((1,), (1,)), ((), ())), preferred_element_type=F32)


def dot_nn(a, b):
    return lax.dot_general(a, b, (((1,), (0,)), ((), ())), preferred_element_type=F32)


def iota(shape, dim):
    return lax.broadcasted_iota(jnp.int32, shape, dim)


def onehot(pred):
    return jnp.where(pred, jnp.float32(1), jnp.float32(0)).astype(BF16)


def await_bytes(ref, sem):
    pltpu.make_async_copy(ref, ref, sem).wait()


def kernel(
    og_h, g_h, u_h, wg_h, wu_h, wd_h, wp_h, eh_h, rt, cnt, out,
    og, wd, wg, wu, wpm, wpp, graw, uraw, eraw, gpad, upad,
    gu, ebuf, hbuf, ra1, s1, s1b, ra2, s2, ra3, hfull, fa, fb,
    xb, rb1, sb, rb2, xfull, ept,
    yb, rc1, c1, rc2, c2, yfull, fin,
    lsem, ssem, rsem,
):
    e, r, c = lax.axis_index("enc"), lax.axis_index("row"), lax.axis_index("col")
    x, core = e // 2, e % 2
    z, yh = r // 2, r % 2

    sib = (x * 2 + (1 - core), r, c)
    other_y = (e, z * 2 + (1 - yh), c)

    def at_x(k):
        return lax.rem(x + k, 4)

    def at_c(k):
        return lax.rem(c + k, 4)

    def at_z(k):
        return lax.rem(z + k, 12)

    def dev_x(k):
        return (at_x(k) * 2 + core, r, c)

    def dev_c(k):
        return (e, r, at_c(k))

    def dev_z(k):
        return (e, at_z(k) * 2 + yh, c)

    totals = {
        0: ra1, 2: ra3, 3: hfull.at[pl.ds(0, 18)],
        5: hfull.at[pl.ds(0, HT // 2)], 6: rb1, 7: rb2, 8: xfull.at[pl.ds(0, 66)], 9: rc1,
        10: gu.at[:, 0, 0], 11: gu.at[:, 0, 0], 12: ebuf.at[0],
        13: ebuf.at[pl.ds(0, 22)], 14: gu.at[:, :, 0], 15: rc2, 16: c2.at[pl.ds(0, 3)],
        17: yfull.at[pl.ds(0, 36)], 18: yfull.at[pl.ds(0, YT // 2)],
    }
    for n in (21, 22):
        totals[n] = gu.at[0, 0, 0]
    for n in range(23, 29):
        totals[n] = hfull.at[pl.ds(0, 12)]
    for n in range(29, 31):
        totals[n] = ra2.at[0, 0]
    for n in range(31, 35):
        totals[n] = ra2.at[0, 0]
    unsent, unread = [], []

    def arrived(n):
        unread.remove(n)
        await_bytes(totals.get(n, fin.at[0, pl.ds(0, CUT)]), rsem.at[n])

    def left(n):
        unsent.remove(n)
        await_bytes(totals.get(n, fin.at[0, pl.ds(0, CUT)]), ssem.at[n])

    def send(src, dst, n, to):
        if n not in unsent:
            unsent.append(n)
            unread.append(n)
        pltpu.make_async_remote_copy(
            src_ref=src, dst_ref=dst, send_sem=ssem.at[n], recv_sem=rsem.at[n],
            device_id=to, device_id_type=MESH,
        ).start()

    def block(ref, base, size, k, h):
        return ref.at[pl.ds(base + at_x(k) * size + h * (size // 2), size // 2)]

    def gather_x(ref, base, size, n):
        for k, h, m in ((1, 0, 0), (3, 1, 1), (1, 1, 2), (3, 0, 3)):
            own = block(ref, base, size, 0, h)
            send(own, own, n + m, dev_x(k))

    def gathered_x(ref, base, size, n):
        arrived(n)
        far = block(ref, base, size, 3, 0)
        send(far, far, n + 4, dev_x(1))
        arrived(n + 1)
        far = block(ref, base, size, 1, 1)
        send(far, far, n + 5, dev_x(3))
        for m in (2, 3, 4, 5):
            arrived(n + m)

    def local(src, dst, n):
        copy = pltpu.make_async_copy(src, dst, lsem.at[n])
        copy.start()
        return copy

    wp_main = wp_h.at[pl.ds(pl.multiple_of(r * 512, 512), 512)]
    wp_tail = wp_h.at[pl.ds(pl.multiple_of(12288 + 32 * jnp.minimum(r, 15), 32), 32)]
    load_og = local(og_h, og, 0)
    load_wd = local(wd_h, wd.at[pl.ds(0, HID)], 1)
    load_g = local(g_h, graw, 2)
    load_u = local(u_h, uraw, 3)
    load_e = local(eh_h, eraw, 4)
    load_wg = local(wg_h, wg.at[pl.ds(0, HID)], 5)
    load_wu = local(wu_h, wu.at[pl.ds(0, HID)], 6)
    load_wm = local(wp_main, wpm.at[pl.ds(0, 512)], 7)
    load_wt = local(wp_tail, wpm.at[pl.ds(512, 32)], 8)

    barrier = pltpu.get_barrier_semaphore()
    pl.semaphore_signal(barrier, inc=1, device_id=sib, device_id_type=MESH)
    pl.semaphore_signal(barrier, inc=1, device_id=other_y, device_id_type=MESH)
    for k in range(1, 4):
        pl.semaphore_signal(barrier, inc=1, device_id=dev_x(k), device_id_type=MESH)
        pl.semaphore_signal(barrier, inc=1, device_id=dev_c(k), device_id_type=MESH)
    for k in range(1, 12):
        pl.semaphore_signal(barrier, inc=1, device_id=dev_z(k), device_id_type=MESH)

    tail = jnp.zeros((HIDP - HID, KD), BF16)
    wd[HID:, :] = tail
    wg[HID:, :] = tail
    wu[HID:, :] = tail
    gpad[...] = jnp.zeros_like(gpad)
    upad[...] = jnp.zeros_like(upad)
    hbuf[ROWT * LT :] = jnp.zeros((HT - ROWT * LT, 16, 128), BF16)
    yb[ROWT * 5 :] = jnp.zeros((YT - ROWT * 5, 16, 128), BF16)
    ebuf[r] = jnp.zeros((48, 256), BF16)

    load_g.wait()
    load_u.wait()
    gpad[0:GR, 0:HID] = graw[...]
    upad[0:GR, 0:HID] = uraw[...]
    row, lane = iota((GRP, 48), 0), iota((GRP, 48), 1)
    pick_g = onehot((row == lane) & (lane < GR))
    pick_u = onehot((row == lane + GR) & (lane < GR))
    stacked = dot_nn(pick_g, gpad[...]) + dot_nn(pick_u, upad[...])
    stacked = stacked.astype(BF16)
    gu[0, x, core] = stacked[:, 0:640]
    gu[1, x, core] = stacked[:, 640:1280]
    load_e.wait()
    ebuf[r, :, 0:EC] = eraw[...]

    load_og.wait()
    load_wd.wait()

    def hidden(j, carry):
        w = wd[pl.ds(pl.multiple_of(j * 128, 128), 128), :]
        part = dot_nt(og[...], w)
        hbuf[pl.ds(j * ROWT, ROWT)] = part.reshape(ROWT, 16, 128).astype(BF16)
        return carry

    lax.fori_loop(0, LT, hidden, 0)

    pl.semaphore_wait(barrier, 19)

    half = HT // 2
    send(hbuf.at[pl.ds((1 - core) * half, half)], ra1, 0, sib)
    send(ebuf.at[r], ebuf.at[r], 12, other_y)
    arrived(0)
    mine = hbuf[pl.ds(core * half, half)].astype(F32) + ra1[...].astype(F32)
    s1[...] = mine.astype(BF16).reshape(4, 2, 12, 16, 128)

    near, far, back = at_x(1), at_x(2), at_x(3)
    send(s1.at[far, 0], ra2.at[0, 0], 29, dev_x(1))
    send(s1.at[far, 1], ra2.at[0, 1], 30, dev_x(3))
    send(s1.at[near, 1], ra2.at[1, 1], 31, dev_x(1))
    send(s1.at[back, 0], ra2.at[2, 0], 32, dev_x(3))
    arrived(29)
    s1b[0] = (s1[near, 0].astype(F32) + ra2[0, 0].astype(F32)).astype(BF16)
    send(s1b.at[0], ra2.at[1, 0], 33, dev_x(1))
    arrived(30)
    s1b[1] = (s1[back, 1].astype(F32) + ra2[0, 1].astype(F32)).astype(BF16)
    send(s1b.at[1], ra2.at[2, 1], 34, dev_x(3))
    send(gu.at[:, x, core], gu.at[:, x, core], 10, dev_x(1))
    send(gu.at[:, x, core], gu.at[:, x, core], 11, dev_x(3))
    arrived(12)
    pair = ebuf.at[pl.ds(2 * z, 2)]
    for k in range(1, 12):
        send(pair, pair, 13, dev_z(k))
    for n in (31, 32, 33, 34):
        arrived(n)
    got = s1[x].astype(F32) + ra2[1].astype(F32) + ra2[2].astype(F32)
    s2[...] = got.astype(BF16).reshape(4, 6, 16, 128)

    for k in range(1, 4):
        send(s2.at[at_c(k)], ra3.at[k - 1], 2, dev_c(k))

    load_wm.wait()
    load_wt.wait()
    for q in range(4):
        move = onehot(iota((128, 512), 1) == 4 * iota((128, 512), 0) + q)
        wpp[q * 128 : (q + 1) * 128, :] = dot_nn(move, wpm[0:512, :]).astype(BF16)
    row, lane = iota((128, 32), 0), iota((128, 32), 1)
    move = onehot((lane == 4 * (row & 7) + (row >> 3)) & (row < 32))
    wpp[512:640, :] = dot_nn(move, wpm[512:544, :]).astype(BF16)

    arrived(2)
    got = s2[c].astype(F32)
    for k in range(3):
        got = got + ra3[k].astype(F32)
    base = core * half + x * 24
    hfull[pl.ds(base + c * 6, 6)] = got.astype(BF16)

    own = hfull.at[pl.ds(base + c * 6, 6)]
    for k in range(1, 4):
        send(own, own, 3, dev_c(k))
    arrived(10)
    send(gu.at[0, at_x(3), core], gu.at[0, at_x(3), core], 21, dev_x(1))
    arrived(11)
    send(gu.at[1, at_x(1), core], gu.at[1, at_x(1), core], 22, dev_x(3))
    arrived(3)
    gather_x(hfull, core * half, 24, 23)
    arrived(21)
    arrived(22)
    send(gu.at[:, :, core], gu.at[:, :, core], 14, sib)

    arrived(14)
    col = iota((NI, 8 * GRP), 1)
    target = col
    for s in range(1, 8):
        target = target - jnp.where(col >= GRP * s, GRP - GR, 0)
    start_of = jnp.zeros_like(col)
    for s in range(1, 8):
        start_of = start_of + jnp.where(col >= GRP * s, GRP, 0)
    within = col - start_of
    row = iota((NI, 8 * GRP), 0)
    place_g = onehot((row == target) & (within < GR))
    place_u = onehot((row == target - GR) & (within >= GR) & (within < 2 * GR))

    for h in range(2):
        def factors(j, carry):
            rows = gu[h, :, :, :, pl.ds(pl.multiple_of(j * 128, 128), 128)]
            rows = rows.reshape(8 * GRP, 128)
            gate = dot_nn(place_g, rows)
            up = dot_nn(place_u, rows)
            squash = 1.0 / (1.0 + jnp.exp(-gate))
            fa[h * 5 + j] = up * squash * (1.0 + gate * (1.0 - squash))
            fb[h * 5 + j] = gate * squash
            return carry

        lax.fori_loop(0, 5, factors, 0)

    gathered_x(hfull, core * half, 24, 23)
    own = hfull.at[pl.ds(core * half, half)]
    send(own, own, 5, sib)
    load_wg.wait()
    load_wu.wait()
    arrived(5)

    def inputs(j, total):
        h = hfull[pl.ds(j * ROWT, ROWT)].astype(F32).reshape(NI, 128)
        cut = pl.ds(pl.multiple_of(j * 128, 128), 128)
        total = total + dot_nn((h * fa[j]).astype(BF16), wg[cut, :])
        return total + dot_nn((h * fb[j]).astype(BF16), wu[cut, :])

    part = lax.fori_loop(0, LT, inputs, jnp.zeros((NI, KD), F32))
    for l in range(2):
        xb[l * 36 : (l + 1) * 36] = part[:, l * 128 : (l + 1) * 128].reshape(36, 8, 128).astype(BF16)

    for k in range(1, 12):
        send(xb.at[pl.ds(at_z(k) * 6, 6)], rb1.at[k - 1], 6, dev_z(k))

    arrived(13)
    lane = iota((1, NI), 1)
    limit = jnp.zeros((1, NI), jnp.int32)
    for s in range(24):
        inside = (lane >= s * IMG) & (lane < (s + 1) * IMG)
        limit = jnp.where(inside, s * IMG + cnt[s], limit)
    slot_row = jnp.where(lane < limit, rt[...].reshape(1, NI), -1)
    routed = onehot(iota((NI, NI), 0) == slot_row)
    et = ebuf[...].reshape(PATCH, 256).astype(F32).T.astype(BF16)
    for q in range(4):
        take = onehot(iota((PATCH, NI), 0) == 4 * iota((PATCH, NI), 1) + q)
        plane = dot_nn(et, take).astype(BF16)
        ept[q] = dot_nt(plane, routed).astype(BF16)

    arrived(6)
    got = xb[pl.ds(z * 6, 6)].astype(F32)
    for k in range(11):
        got = got + rb1[k].astype(F32)
    sb[...] = got.astype(BF16)
    send(sb, rb2, 7, other_y)
    arrived(7)
    xfull[pl.ds(z * 6, 6)] = (sb[...].astype(F32) + rb2[...].astype(F32)).astype(BF16)
    own = xfull.at[pl.ds(z * 6, 6)]
    for k in range(1, 12):
        send(own, own, 8, dev_z(k))
    arrived(8)

    both = xfull[...].astype(F32)
    low = both[0:36].reshape(NI, 128).astype(BF16)
    high = both[36:72].reshape(NI, 128).astype(BF16)
    for q in range(5):
        w = wpp[q * 128 : (q + 1) * 128, :]
        part = dot_nt(low, w[:, 0:128]) + dot_nt(high, w[:, 128:256])
        yb[q * ROWT : (q + 1) * ROWT] = part.reshape(ROWT, 16, 128).astype(BF16)

    half = YT // 2
    send(yb.at[pl.ds((1 - core) * half, half)], rc1, 9, sib)
    arrived(9)
    mine = yb[pl.ds(core * half, half)].astype(F32) + rc1[...].astype(F32)
    c1[...] = mine.astype(BF16).reshape(4, 12, 16, 128)
    for k in range(1, 4):
        send(c1.at[at_x(k)], rc2.at[k - 1], 15, dev_x(k))
    arrived(15)
    got = c1[x].astype(F32)
    for k in range(3):
        got = got + rc2[k].astype(F32)
    c2[c] = got.astype(BF16)
    for k in range(1, 4):
        send(c2.at[c], c2.at[c], 16, dev_c(k))
    arrived(16)
    got = c2[0].astype(F32)
    for k in range(1, 4):
        got = got + c2[k].astype(F32)
    base = core * half + x * 12
    yfull[pl.ds(base, 12)] = got.astype(BF16)
    own = yfull.at[pl.ds(base, 12)]
    for k in range(1, 4):
        send(own, own, 17, dev_x(k))
    arrived(17)
    own = yfull.at[pl.ds(core * half, half)]
    send(own, own, 18, sib)
    arrived(18)

    scale = 1.0 / math.sqrt(PATCH)
    extra = yfull[4 * ROWT : 5 * ROWT].reshape(NI, 128)
    main = jnp.zeros((256, FT), F32)
    small = jnp.zeros((256, FT), F32)
    for q in range(4):
        main = main + dot_nn(ept[q], yfull[q * ROWT : (q + 1) * ROWT].reshape(NI, 128))
        tail = dot_nn(ept[q], extra)
        small = small + (tail if q == 0 else pltpu.roll(tail, 128 - 8 * q, 1))
    fin[r, 0:208] = (main[0:208] * scale).astype(BF16)
    turned = (small * scale).T
    fin[r, 208:224] = jnp.concatenate([turned[0:8, 0:128], turned[0:8, 128:256]], axis=0).astype(BF16)

    def part_of(slot, h):
        return fin.at[slot, pl.ds(h * CUT, CUT)]

    for h in range(2):
        send(part_of(r, h), part_of(r, h), 19 + h, other_y)

    flows = (yh, 1 - yh)

    def hops(h, way):
        return 6 if h == way else 5

    def number(f, h, step, way):
        return 37 + ((f * 2 + h) * 6 + step) * 2 + way

    def slot_at(f, step, way):
        behind = 12 - step if way == 0 else step
        return lax.rem(z + behind, 12) * 2 + flows[f]

    def ring(f, h, step, way):
        piece = part_of(slot_at(f, step, way), h)
        send(piece, piece, number(f, h, step, way), dev_z(1 if way == 0 else 11))

    def place(slot, h):
        lanes = pl.ds(pl.multiple_of(slot * 128, 128), 128)
        low, top = (0, CUT) if h == 0 else (CUT, EC)
        out[low:top, lanes] = fin[slot, low:top]

    def begin(f, h):
        for way in range(2):
            ring(f, h, 0, way)
        place(slot_at(f, 0, 0), h)

    def forward(f, h, step):
        for way in range(2):
            if step < hops(h, way):
                arrived(number(f, h, step, way))
                if step + 1 < hops(h, way):
                    ring(f, h, step + 1, way)
        for way in range(2):
            if step < hops(h, way):
                place(slot_at(f, step + 1, way), h)

    begin(0, 0)
    begin(0, 1)
    for tick in range(6 + LAG + 1):
        for h in range(2):
            if tick == LAG + h:
                arrived(19 + h)
                begin(1, h)
        for h in range(2):
            if tick < 6:
                forward(0, h, tick)
        for h in range(2):
            if 0 <= tick - LAG - h < 6:
                forward(1, h, tick - LAG - h)

    ends = [jnp.concatenate([fin[s, 208:216], fin[s, 216:224]], axis=1).astype(F32) for s in range(16)]
    out[:, 3072:3200] = jnp.concatenate(ends, axis=0).T[0:EC].astype(BF16)

    for n in list(unsent):
        left(n)


def shards(out_grad, gate_pre, up_pre, w_gate, w_up, w_down, w_proj, enc_hidden, route, img_count):
    any_spec = pl.BlockSpec(memory_space=pl.ANY)
    vmem = pltpu.VMEM
    tile = (16, 128)
    n_sem = 37 + 48
    result = pl.pallas_call(
        kernel,
        out_shape=jax.ShapeDtypeStruct((EC, 3200), BF16),
        in_specs=[any_spec] * 8
        + [pl.BlockSpec(memory_space=pltpu.VMEM), pl.BlockSpec(memory_space=pltpu.SMEM)],
        out_specs=pl.BlockSpec(memory_space=pltpu.VMEM),
        scratch_shapes=[
            vmem((NI, KD), BF16),
            vmem((HIDP, KD), BF16),
            vmem((HIDP, KD), BF16),
            vmem((HIDP, KD), BF16),
            vmem((544, KD), BF16),
            vmem((640, KD), BF16),
            vmem((GR, HID), BF16),
            vmem((GR, HID), BF16),
            vmem((48, EC), BF16),
            vmem((48, HIDP), BF16),
            vmem((48, HIDP), BF16),
            vmem((2, 4, 2, GRP, 640), BF16),
            vmem((24, 48, 256), BF16),
            vmem((HT, *tile), BF16),
            vmem((HT // 2, *tile), BF16),
            vmem((4, 2, 12, *tile), BF16),
            vmem((2, 12, *tile), BF16),
            vmem((3, 2, 12, *tile), BF16),
            vmem((4, 6, *tile), BF16),
            vmem((3, 6, *tile), BF16),
            vmem((HT, *tile), BF16),
            vmem((LT, NI, 128), F32),
            vmem((LT, NI, 128), F32),
            vmem((72, 8, 128), BF16),
            vmem((11, 6, 8, 128), BF16),
            vmem((6, 8, 128), BF16),
            vmem((6, 8, 128), BF16),
            vmem((72, 8, 128), BF16),
            vmem((4, 256, NI), BF16),
            vmem((YT, *tile), BF16),
            vmem((YT // 2, *tile), BF16),
            vmem((4, 12, *tile), BF16),
            vmem((3, 12, *tile), BF16),
            vmem((4, 12, *tile), BF16),
            vmem((YT, *tile), BF16),
            vmem((24, PIECE, 128), BF16),
            pltpu.SemaphoreType.DMA((9,)),
            pltpu.SemaphoreType.DMA((n_sem,)),
            pltpu.SemaphoreType.DMA((n_sem,)),
        ],
        compiler_params=pltpu.CompilerParams(
            collective_id=0, has_side_effects=True, vmem_limit_bytes=56 * 1024 * 1024
        ),
    )(
        out_grad, gate_pre, up_pre, w_gate.T, w_up.T, w_down, w_proj, enc_hidden,
        route, img_count,
    )
    return result.T


def solution(mesh):
    placed = (
        P(None, ("enc", "col")),
        P("enc", "row"),
        P("enc", "row"),
        P(("enc", "col"), "row"),
        P(("enc", "col"), "row"),
        P("row", ("enc", "col")),
        P(None, ("enc", "col")),
        P("row", ("enc", "col")),
        P(),
        P(),
    )
    return jax.shard_map(
        shards, mesh=mesh, in_specs=placed, out_specs=P(None, ("enc", "col")), check_vma=False
    )
```

```python
import functools
import math

import jax
import jax.numpy as jnp
from jax import lax
from jax.experimental import pallas as pl
from jax.experimental.pallas import tpu as pltpu
from jax.sharding import PartitionSpec as P

F32 = jnp.float32
BF16 = jnp.bfloat16
MESH = pl.DeviceIdType.MESH

NI = 288
ROWT = NI // 16
KD = 256
HID = 1232
HIDP = 1280
LT = HIDP // 128
GR = 36
GRP = 80
EC = 200
HT = 192
YT = 96
IMG = 12
PATCH = 1152
FT = 128
PIECE = 224
CUT = PIECE // 2
LAG = 1


def dot_nt(a, b):
    return lax.dot_general(a, b, (((1,), (1,)), ((), ())), preferred_element_type=F32)


def dot_nn(a, b):
    return lax.dot_general(a, b, (((1,), (0,)), ((), ())), preferred_element_type=F32)


def iota(shape, dim):
    return lax.broadcasted_iota(jnp.int32, shape, dim)


def onehot(pred):
    return jnp.where(pred, jnp.float32(1), jnp.float32(0)).astype(BF16)


def await_bytes(ref, sem):
    pltpu.make_async_copy(ref, ref, sem).wait()


def kernel(
    og_h, g_h, u_h, wg_h, wu_h, wd_h, wp_h, eh_h, rt, cnt, out,
    og, wd, wg, wu, wpm, wpp, graw, uraw, eraw, gpad, upad,
    gu, ebuf, hbuf, ra1, s1, s1b, ra2, s2, ra3, hfull, fa, fb,
    xb, rb1, sb, rb2, xfull, ept,
    yb, rc1, c1, rc2, c2, yfull, fin,
    lsem, ssem, rsem,
):
    e, r, c = lax.axis_index("enc"), lax.axis_index("row"), lax.axis_index("col")
    x, core = e // 2, e % 2
    z, yh = r // 2, r % 2

    sib = (x * 2 + (1 - core), r, c)
    other_y = (e, z * 2 + (1 - yh), c)

    def at_x(k):
        return lax.rem(x + k, 4)

    def at_c(k):
        return lax.rem(c + k, 4)

    def at_z(k):
        return lax.rem(z + k, 12)

    def dev_x(k):
        return (at_x(k) * 2 + core, r, c)

    def dev_c(k):
        return (e, r, at_c(k))

    def dev_z(k):
        return (e, at_z(k) * 2 + yh, c)

    totals = {
        0: ra1, 2: ra3, 3: hfull.at[pl.ds(0, 18)],
        5: hfull.at[pl.ds(0, HT // 2)], 6: rb1, 7: rb2, 8: xfull.at[pl.ds(0, 66)], 9: rc1,
        10: gu.at[:, 0, 0], 11: gu.at[:, 0, 0], 12: ebuf.at[0],
        13: ebuf.at[pl.ds(0, 22)], 14: gu.at[:, :, 0], 15: rc2, 16: c2.at[pl.ds(0, 3)],
        17: yfull.at[pl.ds(0, 36)], 18: yfull.at[pl.ds(0, YT // 2)],
    }
    for n in (21, 22):
        totals[n] = gu.at[0, 0, 0]
    for n in range(23, 29):
        totals[n] = hfull.at[pl.ds(0, 12)]
    for n in range(29, 31):
        totals[n] = ra2.at[0, 0]
    for n in range(31, 35):
        totals[n] = ra2.at[0, 0]
    unsent, unread = [], []

    def arrived(n):
        unread.remove(n)
        await_bytes(totals.get(n, fin.at[0, pl.ds(0, CUT)]), rsem.at[n])

    def left(n):
        unsent.remove(n)
        await_bytes(totals.get(n, fin.at[0, pl.ds(0, CUT)]), ssem.at[n])

    def send(src, dst, n, to):
        if n not in unsent:
            unsent.append(n)
            unread.append(n)
        pltpu.make_async_remote_copy(
            src_ref=src, dst_ref=dst, send_sem=ssem.at[n], recv_sem=rsem.at[n],
            device_id=to, device_id_type=MESH,
        ).start()

    def block(ref, base, size, k, h):
        return ref.at[pl.ds(base + at_x(k) * size + h * (size // 2), size // 2)]

    def gather_x(ref, base, size, n):
        for k, h, m in ((1, 0, 0), (3, 1, 1), (1, 1, 2), (3, 0, 3)):
            own = block(ref, base, size, 0, h)
            send(own, own, n + m, dev_x(k))

    def gathered_x(ref, base, size, n):
        arrived(n)
        far = block(ref, base, size, 3, 0)
        send(far, far, n + 4, dev_x(1))
        arrived(n + 1)
        far = block(ref, base, size, 1, 1)
        send(far, far, n + 5, dev_x(3))
        for m in (2, 3, 4, 5):
            arrived(n + m)

    def local(src, dst, n):
        copy = pltpu.make_async_copy(src, dst, lsem.at[n])
        copy.start()
        return copy

    wp_main = wp_h.at[pl.ds(pl.multiple_of(r * 512, 512), 512)]
    wp_tail = wp_h.at[pl.ds(pl.multiple_of(12288 + 32 * jnp.minimum(r, 15), 32), 32)]
    load_og = local(og_h, og, 0)
    load_wd = local(wd_h, wd.at[pl.ds(0, HID)], 1)
    load_g = local(g_h, graw, 2)
    load_u = local(u_h, uraw, 3)
    load_e = local(eh_h, eraw, 4)
    load_wg = local(wg_h, wg.at[pl.ds(0, HID)], 5)
    load_wu = local(wu_h, wu.at[pl.ds(0, HID)], 6)
    load_wm = local(wp_main, wpm.at[pl.ds(0, 512)], 7)
    load_wt = local(wp_tail, wpm.at[pl.ds(512, 32)], 8)

    barrier = pltpu.get_barrier_semaphore()
    pl.semaphore_signal(barrier, inc=1, device_id=sib, device_id_type=MESH)
    pl.semaphore_signal(barrier, inc=1, device_id=other_y, device_id_type=MESH)
    for k in range(1, 4):
        pl.semaphore_signal(barrier, inc=1, device_id=dev_x(k), device_id_type=MESH)
        pl.semaphore_signal(barrier, inc=1, device_id=dev_c(k), device_id_type=MESH)
    for k in range(1, 12):
        pl.semaphore_signal(barrier, inc=1, device_id=dev_z(k), device_id_type=MESH)

    tail = jnp.zeros((HIDP - HID, KD), BF16)
    wd[HID:, :] = tail
    wg[HID:, :] = tail
    wu[HID:, :] = tail
    gpad[...] = jnp.zeros_like(gpad)
    upad[...] = jnp.zeros_like(upad)
    hbuf[ROWT * LT :] = jnp.zeros((HT - ROWT * LT, 16, 128), BF16)
    yb[ROWT * 5 :] = jnp.zeros((YT - ROWT * 5, 16, 128), BF16)
    ebuf[r] = jnp.zeros((48, 256), BF16)

    load_g.wait()
    load_u.wait()
    gpad[0:GR, 0:HID] = graw[...]
    upad[0:GR, 0:HID] = uraw[...]
    row, lane = iota((GRP, 48), 0), iota((GRP, 48), 1)
    pick_g = onehot((row == lane) & (lane < GR))
    pick_u = onehot((row == lane + GR) & (lane < GR))
    stacked = dot_nn(pick_g, gpad[...]) + dot_nn(pick_u, upad[...])
    stacked = stacked.astype(BF16)
    gu[0, x, core] = stacked[:, 0:640]
    gu[1, x, core] = stacked[:, 640:1280]
    load_e.wait()
    ebuf[r, :, 0:EC] = eraw[...]

    load_og.wait()
    load_wd.wait()

    def hidden(j, carry):
        w = wd[pl.ds(pl.multiple_of(j * 128, 128), 128), :]
        part = dot_nt(og[...], w)
        hbuf[pl.ds(j * ROWT, ROWT)] = part.reshape(ROWT, 16, 128).astype(BF16)
        return carry

    lax.fori_loop(0, LT, hidden, 0)

    pl.semaphore_wait(barrier, 19)

    half = HT // 2
    send(hbuf.at[pl.ds((1 - core) * half, half)], ra1, 0, sib)
    send(ebuf.at[r], ebuf.at[r], 12, other_y)
    arrived(0)
    mine = hbuf[pl.ds(core * half, half)].astype(F32) + ra1[...].astype(F32)
    s1[...] = mine.astype(BF16).reshape(4, 2, 12, 16, 128)

    near, far, back = at_x(1), at_x(2), at_x(3)
    send(s1.at[far, 0], ra2.at[0, 0], 29, dev_x(1))
    send(s1.at[far, 1], ra2.at[0, 1], 30, dev_x(3))
    send(s1.at[near, 1], ra2.at[1, 1], 31, dev_x(1))
    send(s1.at[back, 0], ra2.at[2, 0], 32, dev_x(3))
    arrived(29)
    s1b[0] = (s1[near, 0].astype(F32) + ra2[0, 0].astype(F32)).astype(BF16)
    send(s1b.at[0], ra2.at[1, 0], 33, dev_x(1))
    arrived(30)
    s1b[1] = (s1[back, 1].astype(F32) + ra2[0, 1].astype(F32)).astype(BF16)
    send(s1b.at[1], ra2.at[2, 1], 34, dev_x(3))
    send(gu.at[:, x, core], gu.at[:, x, core], 10, dev_x(1))
    send(gu.at[:, x, core], gu.at[:, x, core], 11, dev_x(3))
    arrived(12)
    pair = ebuf.at[pl.ds(2 * z, 2)]
    for k in range(1, 12):
        send(pair, pair, 13, dev_z(k))
    for n in (31, 32, 33, 34):
        arrived(n)
    got = s1[x].astype(F32) + ra2[1].astype(F32) + ra2[2].astype(F32)
    s2[...] = got.astype(BF16).reshape(4, 6, 16, 128)

    for k in range(1, 4):
        send(s2.at[at_c(k)], ra3.at[k - 1], 2, dev_c(k))

    load_wm.wait()
    load_wt.wait()
    for q in range(4):
        move = onehot(iota((128, 512), 1) == 4 * iota((128, 512), 0) + q)
        wpp[q * 128 : (q + 1) * 128, :] = dot_nn(move, wpm[0:512, :]).astype(BF16)
    row, lane = iota((128, 32), 0), iota((128, 32), 1)
    move = onehot((lane == 4 * (row & 7) + (row >> 3)) & (row < 32))
    wpp[512:640, :] = dot_nn(move, wpm[512:544, :]).astype(BF16)

    arrived(2)
    got = s2[c].astype(F32)
    for k in range(3):
        got = got + ra3[k].astype(F32)
    base = core * half + x * 24
    hfull[pl.ds(base + c * 6, 6)] = got.astype(BF16)

    own = hfull.at[pl.ds(base + c * 6, 6)]
    for k in range(1, 4):
        send(own, own, 3, dev_c(k))
    arrived(10)
    send(gu.at[0, at_x(3), core], gu.at[0, at_x(3), core], 21, dev_x(1))
    arrived(11)
    send(gu.at[1, at_x(1), core], gu.at[1, at_x(1), core], 22, dev_x(3))
    arrived(3)
    gather_x(hfull, core * half, 24, 23)
    arrived(21)
    arrived(22)
    send(gu.at[:, :, core], gu.at[:, :, core], 14, sib)

    arrived(14)
    col = iota((NI, 8 * GRP), 1)
    target = col
    for s in range(1, 8):
        target = target - jnp.where(col >= GRP * s, GRP - GR, 0)
    start_of = jnp.zeros_like(col)
    for s in range(1, 8):
        start_of = start_of + jnp.where(col >= GRP * s, GRP, 0)
    within = col - start_of
    row = iota((NI, 8 * GRP), 0)
    place_g = onehot((row == target) & (within < GR))
    place_u = onehot((row == target - GR) & (within >= GR) & (within < 2 * GR))

    for h in range(2):
        def factors(j, carry):
            rows = gu[h, :, :, :, pl.ds(pl.multiple_of(j * 128, 128), 128)]
            rows = rows.reshape(8 * GRP, 128)
            gate = dot_nn(place_g, rows)
            up = dot_nn(place_u, rows)
            squash = 1.0 / (1.0 + jnp.exp(-gate))
            fa[h * 5 + j] = up * squash * (1.0 + gate * (1.0 - squash))
            fb[h * 5 + j] = gate * squash
            return carry

        lax.fori_loop(0, 5, factors, 0)

    gathered_x(hfull, core * half, 24, 23)
    own = hfull.at[pl.ds(core * half, half)]
    send(own, own, 5, sib)
    load_wg.wait()
    load_wu.wait()
    arrived(5)

    def inputs(j, total):
        h = hfull[pl.ds(j * ROWT, ROWT)].astype(F32).reshape(NI, 128)
        cut = pl.ds(pl.multiple_of(j * 128, 128), 128)
        total = total + dot_nn((h * fa[j]).astype(BF16), wg[cut, :])
        return total + dot_nn((h * fb[j]).astype(BF16), wu[cut, :])

    part = lax.fori_loop(0, LT, inputs, jnp.zeros((NI, KD), F32))
    for l in range(2):
        xb[l * 36 : (l + 1) * 36] = part[:, l * 128 : (l + 1) * 128].reshape(36, 8, 128).astype(BF16)

    for k in range(1, 12):
        send(xb.at[pl.ds(at_z(k) * 6, 6)], rb1.at[k - 1], 6, dev_z(k))

    arrived(13)
    lane = iota((1, NI), 1)
    limit = jnp.zeros((1, NI), jnp.int32)
    for s in range(24):
        inside = (lane >= s * IMG) & (lane < (s + 1) * IMG)
        limit = jnp.where(inside, s * IMG + cnt[s], limit)
    slot_row = jnp.where(lane < limit, rt[...].reshape(1, NI), -1)
    routed = onehot(iota((NI, NI), 0) == slot_row)
    et = ebuf[...].reshape(PATCH, 256).astype(F32).T.astype(BF16)
    for q in range(4):
        take = onehot(iota((PATCH, NI), 0) == 4 * iota((PATCH, NI), 1) + q)
        plane = dot_nn(et, take).astype(BF16)
        ept[q] = dot_nt(plane, routed).astype(BF16)

    arrived(6)
    got = xb[pl.ds(z * 6, 6)].astype(F32)
    for k in range(11):
        got = got + rb1[k].astype(F32)
    sb[...] = got.astype(BF16)
    send(sb, rb2, 7, other_y)
    arrived(7)
    xfull[pl.ds(z * 6, 6)] = (sb[...].astype(F32) + rb2[...].astype(F32)).astype(BF16)
    own = xfull.at[pl.ds(z * 6, 6)]
    for k in range(1, 12):
        send(own, own, 8, dev_z(k))
    arrived(8)

    both = xfull[...].astype(F32)
    low = both[0:36].reshape(NI, 128).astype(BF16)
    high = both[36:72].reshape(NI, 128).astype(BF16)
    for q in range(5):
        w = wpp[q * 128 : (q + 1) * 128, :]
        part = dot_nt(low, w[:, 0:128]) + dot_nt(high, w[:, 128:256])
        yb[q * ROWT : (q + 1) * ROWT] = part.reshape(ROWT, 16, 128).astype(BF16)

    half = YT // 2
    send(yb.at[pl.ds((1 - core) * half, half)], rc1, 9, sib)
    arrived(9)
    mine = yb[pl.ds(core * half, half)].astype(F32) + rc1[...].astype(F32)
    c1[...] = mine.astype(BF16).reshape(4, 12, 16, 128)
    for k in range(1, 4):
        send(c1.at[at_x(k)], rc2.at[k - 1], 15, dev_x(k))
    arrived(15)
    got = c1[x].astype(F32)
    for k in range(3):
        got = got + rc2[k].astype(F32)
    c2[c] = got.astype(BF16)
    for k in range(1, 4):
        send(c2.at[c], c2.at[c], 16, dev_c(k))
    arrived(16)
    got = c2[0].astype(F32)
    for k in range(1, 4):
        got = got + c2[k].astype(F32)
    base = core * half + x * 12
    yfull[pl.ds(base, 12)] = got.astype(BF16)
    own = yfull.at[pl.ds(base, 12)]
    for k in range(1, 4):
        send(own, own, 17, dev_x(k))
    arrived(17)
    own = yfull.at[pl.ds(core * half, half)]
    send(own, own, 18, sib)
    arrived(18)

    scale = 1.0 / math.sqrt(PATCH)
    extra = yfull[4 * ROWT : 5 * ROWT].reshape(NI, 128)
    main = jnp.zeros((256, FT), F32)
    small = jnp.zeros((256, FT), F32)
    for q in range(4):
        main = main + dot_nn(ept[q], yfull[q * ROWT : (q + 1) * ROWT].reshape(NI, 128))
        tail = dot_nn(ept[q], extra)
        small = small + (tail if q == 0 else pltpu.roll(tail, 128 - 8 * q, 1))
    fin[r, 0:208] = (main[0:208] * scale).astype(BF16)
    turned = (small * scale).T
    fin[r, 208:224] = jnp.concatenate([turned[0:8, 0:128], turned[0:8, 128:256]], axis=0).astype(BF16)

    def part_of(slot, h):
        return fin.at[slot, pl.ds(h * CUT, CUT)]

    for h in range(2):
        send(part_of(r, h), part_of(r, h), 19 + h, other_y)

    flows = (yh, 1 - yh)

    def hops(h, way):
        return 6 if h == way else 5

    def number(f, h, step, way):
        return 37 + ((f * 2 + h) * 6 + step) * 2 + way

    def slot_at(f, away, way):
        behind = 12 - away if way == 0 else away
        return lax.rem(z + behind, 12) * 2 + flows[f]

    def ring(f, h, away, way):
        piece = part_of(slot_at(f, away, way), h)
        for jump in (2, 1):
            if away + jump <= hops(h, way):
                to = dev_z(jump if way == 0 else 12 - jump)
                send(piece, piece, number(f, h, away + jump - 1, way), to)

    def place(slot, h):
        lanes = pl.ds(pl.multiple_of(slot * 128, 128), 128)
        low, top = (0, CUT) if h == 0 else (CUT, EC)
        out[low:top, lanes] = fin[slot, low:top]

    def begin(f, h):
        for way in range(2):
            ring(f, h, 0, way)
        place(slot_at(f, 0, 0), h)

    def forward(f, h, tick):
        for away in (2 * tick + 2, 2 * tick + 1):
            for way in range(2):
                if away <= hops(h, way):
                    arrived(number(f, h, away - 1, way))
                    if away % 2 == 0:
                        ring(f, h, away, way)
            for way in range(2):
                if away <= hops(h, way):
                    place(slot_at(f, away, way), h)

    begin(0, 0)
    begin(0, 1)
    for tick in range(3 + LAG):
        if tick == LAG:
            for h in range(2):
                arrived(19 + h)
                begin(1, h)
        for h in range(2):
            if tick < 3:
                forward(0, h, tick)
        for h in range(2):
            if tick >= LAG:
                forward(1, h, tick - LAG)

    ends = [jnp.concatenate([fin[s, 208:216], fin[s, 216:224]], axis=1).astype(F32) for s in range(16)]
    out[:, 3072:3200] = jnp.concatenate(ends, axis=0).T[0:EC].astype(BF16)

    for n in list(unsent):
        left(n)


def shards(out_grad, gate_pre, up_pre, w_gate, w_up, w_down, w_proj, enc_hidden, route, img_count):
    any_spec = pl.BlockSpec(memory_space=pltpu.HBM)
    vmem = pltpu.VMEM
    tile = (16, 128)
    n_sem = 37 + 48
    result = pl.pallas_call(
        kernel,
        out_shape=jax.ShapeDtypeStruct((EC, 3200), BF16),
        in_specs=[any_spec] * 8
        + [pl.BlockSpec(memory_space=pltpu.VMEM), pl.BlockSpec(memory_space=pltpu.SMEM)],
        out_specs=pl.BlockSpec(memory_space=pltpu.VMEM),
        scratch_shapes=[
            vmem((NI, KD), BF16),
            vmem((HIDP, KD), BF16),
            vmem((HIDP, KD), BF16),
            vmem((HIDP, KD), BF16),
            vmem((544, KD), BF16),
            vmem((640, KD), BF16),
            vmem((GR, HID), BF16),
            vmem((GR, HID), BF16),
            vmem((48, EC), BF16),
            vmem((48, HIDP), BF16),
            vmem((48, HIDP), BF16),
            vmem((2, 4, 2, GRP, 640), BF16),
            vmem((24, 48, 256), BF16),
            vmem((HT, *tile), BF16),
            vmem((HT // 2, *tile), BF16),
            vmem((4, 2, 12, *tile), BF16),
            vmem((2, 12, *tile), BF16),
            vmem((3, 2, 12, *tile), BF16),
            vmem((4, 6, *tile), BF16),
            vmem((3, 6, *tile), BF16),
            vmem((HT, *tile), BF16),
            vmem((LT, NI, 128), F32),
            vmem((LT, NI, 128), F32),
            vmem((72, 8, 128), BF16),
            vmem((11, 6, 8, 128), BF16),
            vmem((6, 8, 128), BF16),
            vmem((6, 8, 128), BF16),
            vmem((72, 8, 128), BF16),
            vmem((4, 256, NI), BF16),
            vmem((YT, *tile), BF16),
            vmem((YT // 2, *tile), BF16),
            vmem((4, 12, *tile), BF16),
            vmem((3, 12, *tile), BF16),
            vmem((4, 12, *tile), BF16),
            vmem((YT, *tile), BF16),
            vmem((24, PIECE, 128), BF16),
            pltpu.SemaphoreType.DMA((9,)),
            pltpu.SemaphoreType.DMA((n_sem,)),
            pltpu.SemaphoreType.DMA((n_sem,)),
        ],
        compiler_params=pltpu.CompilerParams(
            collective_id=0, has_side_effects=True, vmem_limit_bytes=56 * 1024 * 1024
        ),
    )(
        out_grad, gate_pre, up_pre, w_gate.T, w_up.T, w_down, w_proj, enc_hidden,
        route, img_count,
    )
    return result.T


def solution(mesh):
    placed = (
        P(None, ("enc", "col")),
        P("enc", "row"),
        P("enc", "row"),
        P(("enc", "col"), "row"),
        P(("enc", "col"), "row"),
        P("row", ("enc", "col")),
        P(None, ("enc", "col")),
        P("row", ("enc", "col")),
        P(),
        P(),
    )
    return jax.shard_map(
        shards, mesh=mesh, in_specs=placed, out_specs=P(None, ("enc", "col")), check_vma=False
    )
```

```python
import functools
import math

import jax
import jax.numpy as jnp
from jax import lax
from jax.experimental import pallas as pl
from jax.experimental.pallas import tpu as pltpu
from jax.sharding import PartitionSpec as P

F32 = jnp.float32
BF16 = jnp.bfloat16
MESH = pl.DeviceIdType.MESH

NI = 288
ROWT = NI // 16
KD = 256
HID = 1232
HIDP = 1280
LT = HIDP // 128
GR = 36
GRP = 80
EC = 200
HT = 192
YT = 96
IMG = 12
PATCH = 1152
FT = 128
PIECE = 224
CUT = PIECE // 2


def dot_nt(a, b):
    return lax.dot_general(a, b, (((1,), (1,)), ((), ())), preferred_element_type=F32)


def dot_nn(a, b):
    return lax.dot_general(a, b, (((1,), (0,)), ((), ())), preferred_element_type=F32)


def iota(shape, dim):
    return lax.broadcasted_iota(jnp.int32, shape, dim)


def onehot(pred):
    return jnp.where(pred, jnp.float32(1), jnp.float32(0)).astype(BF16)


def await_bytes(ref, sem):
    pltpu.make_async_copy(ref, ref, sem).wait()


def kernel(
    og_h, g_h, u_h, wg_h, wu_h, wd_h, wp_h, eh_h, rt, cnt, out,
    og, wd, wg, wu, wpm, wpp, graw, uraw, eraw, gpad, upad,
    gu, ebuf, hbuf, ra1, s1, s1b, ra2, s2, ra3, hfull, fa, fb,
    xb, rb1, sb, rb2, xfull, ept,
    yb, rc1, c1, rc2, c2, yfull, fin, last,
    lsem, ssem, rsem,
):
    e, r, c = lax.axis_index("enc"), lax.axis_index("row"), lax.axis_index("col")
    x, core = e // 2, e % 2
    z, yh = r // 2, r % 2

    sib = (x * 2 + (1 - core), r, c)
    other_y = (e, z * 2 + (1 - yh), c)

    def at_x(k):
        return lax.rem(x + k, 4)

    def at_c(k):
        return lax.rem(c + k, 4)

    def at_z(k):
        return lax.rem(z + k, 12)

    def dev_x(k):
        return (at_x(k) * 2 + core, r, c)

    def dev_c(k):
        return (e, r, at_c(k))

    def dev_z(k):
        return (e, at_z(k) * 2 + yh, c)

    totals = {
        0: ra1, 2: ra3, 3: hfull.at[pl.ds(0, 18)],
        5: hfull.at[pl.ds(0, HT // 2)], 6: rb1, 7: rb2, 8: xfull.at[pl.ds(0, 66)], 9: rc1,
        10: gu.at[:, 0, 0], 11: gu.at[:, 0, 0], 12: ebuf.at[0],
        13: ebuf.at[pl.ds(0, 22)], 14: gu.at[:, :, 0], 15: rc2, 16: c2.at[pl.ds(0, 3)],
        17: yfull.at[pl.ds(0, 36)], 18: yfull.at[pl.ds(0, YT // 2)],
    }
    for n in (21, 22):
        totals[n] = gu.at[0, 0, 0]
    for n in range(23, 29):
        totals[n] = hfull.at[pl.ds(0, 12)]
    for n in range(29, 31):
        totals[n] = ra2.at[0, 0]
    for n in range(31, 35):
        totals[n] = ra2.at[0, 0]
    unsent, unread = [], []

    def arrived(n):
        unread.remove(n)
        await_bytes(totals.get(n, fin.at[0, pl.ds(0, CUT)]), rsem.at[n])

    def left(n):
        unsent.remove(n)
        await_bytes(totals.get(n, fin.at[0, pl.ds(0, CUT)]), ssem.at[n])

    def send(src, dst, n, to):
        if n not in unsent:
            unsent.append(n)
            unread.append(n)
        pltpu.make_async_remote_copy(
            src_ref=src, dst_ref=dst, send_sem=ssem.at[n], recv_sem=rsem.at[n],
            device_id=to, device_id_type=MESH,
        ).start()

    def block(ref, base, size, k, h):
        return ref.at[pl.ds(base + at_x(k) * size + h * (size // 2), size // 2)]

    def gather_x(ref, base, size, n):
        for k, h, m in ((1, 0, 0), (3, 1, 1), (1, 1, 2), (3, 0, 3)):
            own = block(ref, base, size, 0, h)
            send(own, own, n + m, dev_x(k))

    def relay_x(ref, base, size, n):
        arrived(n)
        far = block(ref, base, size, 3, 0)
        send(far, far, n + 4, dev_x(1))
        arrived(n + 1)
        far = block(ref, base, size, 1, 1)
        send(far, far, n + 5, dev_x(3))

    def local(src, dst, n):
        copy = pltpu.make_async_copy(src, dst, lsem.at[n])
        copy.start()
        return copy

    wp_main = wp_h.at[pl.ds(pl.multiple_of(r * 512, 512), 512)]
    wp_tail = wp_h.at[pl.ds(pl.multiple_of(12288 + 32 * jnp.minimum(r, 15), 32), 32)]
    load_og = local(og_h, og, 0)
    load_wd = local(wd_h, wd.at[pl.ds(0, HID)], 1)
    load_g = local(g_h, graw, 2)
    load_u = local(u_h, uraw, 3)
    load_e = local(eh_h, eraw, 4)
    load_wg = local(wg_h, wg.at[pl.ds(0, HID)], 5)
    load_wu = local(wu_h, wu.at[pl.ds(0, HID)], 6)
    load_wm = local(wp_main, wpm.at[pl.ds(0, 512)], 7)
    load_wt = local(wp_tail, wpm.at[pl.ds(512, 32)], 8)

    barrier = pltpu.get_barrier_semaphore()
    pl.semaphore_signal(barrier, inc=1, device_id=sib, device_id_type=MESH)
    pl.semaphore_signal(barrier, inc=1, device_id=other_y, device_id_type=MESH)
    for k in range(1, 4):
        pl.semaphore_signal(barrier, inc=1, device_id=dev_x(k), device_id_type=MESH)
        pl.semaphore_signal(barrier, inc=1, device_id=dev_c(k), device_id_type=MESH)
    for k in range(1, 12):
        pl.semaphore_signal(barrier, inc=1, device_id=dev_z(k), device_id_type=MESH)

    tail = jnp.zeros((HIDP - HID, KD), BF16)
    wd[HID:, :] = tail
    wg[HID:, :] = tail
    wu[HID:, :] = tail
    gpad[...] = jnp.zeros_like(gpad)
    upad[...] = jnp.zeros_like(upad)
    hbuf[ROWT * LT :] = jnp.zeros((HT - ROWT * LT, 16, 128), BF16)
    yb[ROWT * 5 :] = jnp.zeros((YT - ROWT * 5, 16, 128), BF16)
    ebuf[r] = jnp.zeros((48, 256), BF16)

    load_g.wait()
    load_u.wait()
    gpad[0:GR, 0:HID] = graw[...]
    upad[0:GR, 0:HID] = uraw[...]
    row, lane = iota((GRP, 48), 0), iota((GRP, 48), 1)
    pick_g = onehot((row == lane) & (lane < GR))
    pick_u = onehot((row == lane + GR) & (lane < GR))
    stacked = dot_nn(pick_g, gpad[...]) + dot_nn(pick_u, upad[...])
    stacked = stacked.astype(BF16)
    gu[0, x, core] = stacked[:, 0:640]
    gu[1, x, core] = stacked[:, 640:1280]
    load_e.wait()
    ebuf[r, :, 0:EC] = eraw[...]

    load_og.wait()
    load_wd.wait()

    def hidden(j, carry):
        w = wd[pl.ds(pl.multiple_of(j * 128, 128), 128), :]
        part = dot_nt(og[...], w)
        hbuf[pl.ds(j * ROWT, ROWT)] = part.reshape(ROWT, 16, 128).astype(BF16)
        return carry

    lax.fori_loop(0, LT, hidden, 0)

    pl.semaphore_wait(barrier, 19)

    half = HT // 2
    send(hbuf.at[pl.ds((1 - core) * half, half)], ra1, 0, sib)
    send(ebuf.at[r], ebuf.at[r], 12, other_y)
    arrived(0)
    mine = hbuf[pl.ds(core * half, half)].astype(F32) + ra1[...].astype(F32)
    s1[...] = mine.astype(BF16).reshape(4, 2, 12, 16, 128)

    near, far, back = at_x(1), at_x(2), at_x(3)
    send(s1.at[far, 0], ra2.at[0, 0], 29, dev_x(1))
    send(s1.at[far, 1], ra2.at[0, 1], 30, dev_x(3))
    send(s1.at[near, 1], ra2.at[1, 1], 31, dev_x(1))
    send(s1.at[back, 0], ra2.at[2, 0], 32, dev_x(3))
    arrived(29)
    s1b[0] = (s1[near, 0].astype(F32) + ra2[0, 0].astype(F32)).astype(BF16)
    send(s1b.at[0], ra2.at[1, 0], 33, dev_x(1))
    arrived(30)
    s1b[1] = (s1[back, 1].astype(F32) + ra2[0, 1].astype(F32)).astype(BF16)
    send(s1b.at[1], ra2.at[2, 1], 34, dev_x(3))
    send(gu.at[:, x, core], gu.at[:, x, core], 10, dev_x(1))
    send(gu.at[:, x, core], gu.at[:, x, core], 11, dev_x(3))
    arrived(12)
    pair = ebuf.at[pl.ds(2 * z, 2)]
    for k in range(1, 12):
        send(pair, pair, 13, dev_z(k))
    for n in (31, 32, 33, 34):
        arrived(n)
    got = s1[x].astype(F32) + ra2[1].astype(F32) + ra2[2].astype(F32)
    s2[...] = got.astype(BF16).reshape(4, 6, 16, 128)

    for k in range(1, 4):
        send(s2.at[at_c(k)], ra3.at[k - 1], 2, dev_c(k))

    load_wm.wait()
    load_wt.wait()
    for q in range(4):
        move = onehot(iota((128, 512), 1) == 4 * iota((128, 512), 0) + q)
        wpp[q * 128 : (q + 1) * 128, :] = dot_nn(move, wpm[0:512, :]).astype(BF16)
    row, lane = iota((128, 32), 0), iota((128, 32), 1)
    move = onehot((lane == 4 * (row & 7) + (row >> 3)) & (row < 32))
    wpp[512:640, :] = dot_nn(move, wpm[512:544, :]).astype(BF16)

    arrived(2)
    got = s2[c].astype(F32)
    for k in range(3):
        got = got + ra3[k].astype(F32)
    base = core * half + x * 24
    hfull[pl.ds(base + c * 6, 6)] = got.astype(BF16)

    own = hfull.at[pl.ds(base + c * 6, 6)]
    for k in range(1, 4):
        send(own, own, 3, dev_c(k))
    arrived(10)
    send(gu.at[0, at_x(3), core], gu.at[0, at_x(3), core], 21, dev_x(1))
    arrived(11)
    send(gu.at[1, at_x(1), core], gu.at[1, at_x(1), core], 22, dev_x(3))
    arrived(3)
    gather_x(hfull, core * half, 24, 23)
    arrived(21)
    arrived(22)
    send(gu.at[:, :, core], gu.at[:, :, core], 14, sib)
    relay_x(hfull, core * half, 24, 23)

    arrived(14)
    col = iota((NI, 8 * GRP), 1)
    target = col
    for s in range(1, 8):
        target = target - jnp.where(col >= GRP * s, GRP - GR, 0)
    start_of = jnp.zeros_like(col)
    for s in range(1, 8):
        start_of = start_of + jnp.where(col >= GRP * s, GRP, 0)
    within = col - start_of
    row = iota((NI, 8 * GRP), 0)
    place_g = onehot((row == target) & (within < GR))
    place_u = onehot((row == target - GR) & (within >= GR) & (within < 2 * GR))

    for h in range(2):
        def factors(j, carry):
            rows = gu[h, :, :, :, pl.ds(pl.multiple_of(j * 128, 128), 128)]
            rows = rows.reshape(8 * GRP, 128)
            gate = dot_nn(place_g, rows)
            up = dot_nn(place_u, rows)
            squash = 1.0 / (1.0 + jnp.exp(-gate))
            fa[h * 5 + j] = up * squash * (1.0 + gate * (1.0 - squash))
            fb[h * 5 + j] = gate * squash
            return carry

        lax.fori_loop(0, 5, factors, 0)

    for n in (25, 26, 27, 28):
        arrived(n)
    own = hfull.at[pl.ds(core * half, half)]
    send(own, own, 5, sib)
    load_wg.wait()
    load_wu.wait()
    arrived(5)

    def inputs(j, total):
        h = hfull[pl.ds(j * ROWT, ROWT)].astype(F32).reshape(NI, 128)
        cut = pl.ds(pl.multiple_of(j * 128, 128), 128)
        total = total + dot_nn((h * fa[j]).astype(BF16), wg[cut, :])
        return total + dot_nn((h * fb[j]).astype(BF16), wu[cut, :])

    part = lax.fori_loop(0, LT, inputs, jnp.zeros((NI, KD), F32))
    for l in range(2):
        xb[l * 36 : (l + 1) * 36] = part[:, l * 128 : (l + 1) * 128].reshape(36, 8, 128).astype(BF16)

    for k in range(1, 12):
        send(xb.at[pl.ds(at_z(k) * 6, 6)], rb1.at[k - 1], 6, dev_z(k))

    arrived(13)
    lane = iota((1, NI), 1)
    limit = jnp.zeros((1, NI), jnp.int32)
    for s in range(24):
        inside = (lane >= s * IMG) & (lane < (s + 1) * IMG)
        limit = jnp.where(inside, s * IMG + cnt[s], limit)
    slot_row = jnp.where(lane < limit, rt[...].reshape(1, NI), -1)
    routed = onehot(iota((NI, NI), 0) == slot_row)
    et = ebuf[...].reshape(PATCH, 256).astype(F32).T.astype(BF16)
    for q in range(4):
        take = onehot(iota((PATCH, NI), 0) == 4 * iota((PATCH, NI), 1) + q)
        plane = dot_nn(et, take).astype(BF16)
        ept[q] = dot_nt(plane, routed).astype(BF16)

    arrived(6)
    got = xb[pl.ds(z * 6, 6)].astype(F32)
    for k in range(11):
        got = got + rb1[k].astype(F32)
    sb[...] = got.astype(BF16)
    send(sb, rb2, 7, other_y)
    arrived(7)
    xfull[pl.ds(z * 6, 6)] = (sb[...].astype(F32) + rb2[...].astype(F32)).astype(BF16)
    own = xfull.at[pl.ds(z * 6, 6)]
    for k in range(1, 12):
        send(own, own, 8, dev_z(k))
    arrived(8)

    both = xfull[...].astype(F32)
    low = both[0:36].reshape(NI, 128).astype(BF16)
    high = both[36:72].reshape(NI, 128).astype(BF16)
    for q in range(5):
        w = wpp[q * 128 : (q + 1) * 128, :]
        part = dot_nt(low, w[:, 0:128]) + dot_nt(high, w[:, 128:256])
        yb[q * ROWT : (q + 1) * ROWT] = part.reshape(ROWT, 16, 128).astype(BF16)

    half = YT // 2
    send(yb.at[pl.ds((1 - core) * half, half)], rc1, 9, sib)
    arrived(9)
    mine = yb[pl.ds(core * half, half)].astype(F32) + rc1[...].astype(F32)
    c1[...] = mine.astype(BF16).reshape(4, 12, 16, 128)
    for k in range(1, 4):
        send(c1.at[at_x(k)], rc2.at[k - 1], 15, dev_x(k))
    arrived(15)
    got = c1[x].astype(F32)
    for k in range(3):
        got = got + rc2[k].astype(F32)
    c2[c] = got.astype(BF16)
    for k in range(1, 4):
        send(c2.at[c], c2.at[c], 16, dev_c(k))
    arrived(16)
    got = c2[0].astype(F32)
    for k in range(1, 4):
        got = got + c2[k].astype(F32)
    base = core * half + x * 12
    yfull[pl.ds(base, 12)] = got.astype(BF16)
    own = yfull.at[pl.ds(base, 12)]
    for k in range(1, 4):
        send(own, own, 17, dev_x(k))
    arrived(17)
    own = yfull.at[pl.ds(core * half, half)]
    send(own, own, 18, sib)
    arrived(18)

    scale = 1.0 / math.sqrt(PATCH)
    extra = yfull[4 * ROWT : 5 * ROWT].reshape(NI, 128)
    main = jnp.zeros((256, FT), F32)
    small = jnp.zeros((256, FT), F32)
    for q in range(4):
        main = main + dot_nn(ept[q], yfull[q * ROWT : (q + 1) * ROWT].reshape(NI, 128))
        tail = dot_nn(ept[q], extra)
        small = small + (tail if q == 0 else pltpu.roll(tail, 128 - 8 * q, 1))
    fin[r, 0:208] = (main[0:208] * scale).astype(BF16)
    turned = (small * scale).T
    fin[r, 208:224] = jnp.concatenate([turned[0:8, 0:128], turned[0:8, 128:256]], axis=0).astype(BF16)

    def part_of(slot, h):
        return fin.at[slot, pl.ds(h * CUT, CUT)]

    for h in range(2):
        send(part_of(r, h), part_of(r, h), 19 + h, other_y)

    flows = (yh, 1 - yh)

    def hops(h, way):
        return 6 if h == way else 5

    def number(f, h, step, way):
        return 37 + ((f * 2 + h) * 6 + step) * 2 + way

    def slot_at(f, away, way):
        behind = 12 - away if way == 0 else away
        return lax.rem(z + behind, 12) * 2 + flows[f]

    def jumps(f, away):
        return (1,) if f == 0 else ((2, 1) if away % 2 == 0 else ())

    def ring(f, h, away, way):
        piece = part_of(slot_at(f, away, way), h)
        for jump in jumps(f, away):
            if away + jump <= hops(h, way):
                to = dev_z(jump if way == 0 else 12 - jump)
                send(piece, piece, number(f, h, away + jump - 1, way), to)

    def place(slot, h):
        lanes = pl.ds(pl.multiple_of(slot * 128, 128), 128)
        low, top = (0, CUT) if h == 0 else (CUT, EC)
        pltpu.make_async_copy(
            fin.at[slot, pl.ds(low, top - low)], out.at[pl.ds(low, top - low), lanes], lsem.at[9]
        ).start()

    def begin(f, h):
        for way in range(2):
            ring(f, h, 0, way)
        place(slot_at(f, 0, 0), h)

    def forward(f, h, away):
        for way in range(2):
            if away <= hops(h, way):
                arrived(number(f, h, away - 1, way))
                ring(f, h, away, way)
        for way in range(2):
            if away <= hops(h, way):
                place(slot_at(f, away, way), h)

    begin(0, 0)
    begin(0, 1)
    order = ((0, 1), (0, 2), (1, 0), (0, 3), (1, 2), (1, 1), (0, 4), (1, 4), (0, 5), (1, 3), (0, 6), (1, 6), (1, 5))
    for f, away in order:
        for h in range(2):
            if away == 0:
                arrived(19 + h)
                begin(f, h)
            else:
                forward(f, h, away)

    ends = [jnp.concatenate([fin[s, 208:216], fin[s, 216:224]], axis=1).astype(F32) for s in range(16)]
    last[...] = jnp.concatenate(ends, axis=0).T[0:EC].astype(BF16)
    local(last, out.at[:, pl.ds(3072, 128)], 10).wait()
    await_bytes(out.at[:, pl.ds(0, 3072)], lsem.at[9])

    for n in list(unsent):
        left(n)


def shards(out_grad, gate_pre, up_pre, w_gate, w_up, w_down, w_proj, enc_hidden, route, img_count):
    any_spec = pl.BlockSpec(memory_space=pltpu.HBM)
    vmem = pltpu.VMEM
    tile = (16, 128)
    n_sem = 37 + 48
    result = pl.pallas_call(
        kernel,
        out_shape=jax.ShapeDtypeStruct((EC, 3200), BF16),
        in_specs=[any_spec] * 8
        + [pl.BlockSpec(memory_space=pltpu.VMEM), pl.BlockSpec(memory_space=pltpu.SMEM)],
        out_specs=any_spec,
        scratch_shapes=[
            vmem((NI, KD), BF16),
            vmem((HIDP, KD), BF16),
            vmem((HIDP, KD), BF16),
            vmem((HIDP, KD), BF16),
            vmem((544, KD), BF16),
            vmem((640, KD), BF16),
            vmem((GR, HID), BF16),
            vmem((GR, HID), BF16),
            vmem((48, EC), BF16),
            vmem((48, HIDP), BF16),
            vmem((48, HIDP), BF16),
            vmem((2, 4, 2, GRP, 640), BF16),
            vmem((24, 48, 256), BF16),
            vmem((HT, *tile), BF16),
            vmem((HT // 2, *tile), BF16),
            vmem((4, 2, 12, *tile), BF16),
            vmem((2, 12, *tile), BF16),
            vmem((3, 2, 12, *tile), BF16),
            vmem((4, 6, *tile), BF16),
            vmem((3, 6, *tile), BF16),
            vmem((HT, *tile), BF16),
            vmem((LT, NI, 128), F32),
            vmem((LT, NI, 128), F32),
            vmem((72, 8, 128), BF16),
            vmem((11, 6, 8, 128), BF16),
            vmem((6, 8, 128), BF16),
            vmem((6, 8, 128), BF16),
            vmem((72, 8, 128), BF16),
            vmem((4, 256, NI), BF16),
            vmem((YT, *tile), BF16),
            vmem((YT // 2, *tile), BF16),
            vmem((4, 12, *tile), BF16),
            vmem((3, 12, *tile), BF16),
            vmem((4, 12, *tile), BF16),
            vmem((YT, *tile), BF16),
            vmem((24, PIECE, 128), BF16),
            vmem((EC, 128), BF16),
            pltpu.SemaphoreType.DMA((11,)),
            pltpu.SemaphoreType.DMA((n_sem,)),
            pltpu.SemaphoreType.DMA((n_sem,)),
        ],
        compiler_params=pltpu.CompilerParams(
            collective_id=0, has_side_effects=True, vmem_limit_bytes=56 * 1024 * 1024
        ),
    )(
        out_grad, gate_pre, up_pre, w_gate.T, w_up.T, w_down, w_proj, enc_hidden,
        route, img_count,
    )
    return result.T


def solution(mesh):
    placed = (
        P(None, ("enc", "col")),
        P("enc", "row"),
        P("enc", "row"),
        P(("enc", "col"), "row"),
        P(("enc", "col"), "row"),
        P("row", ("enc", "col")),
        P(None, ("enc", "col")),
        P("row", ("enc", "col")),
        P(),
        P(),
    )
    return jax.shard_map(
        shards, mesh=mesh, in_specs=placed, out_specs=P(None, ("enc", "col")), check_vma=False
    )
```
